32 devices in a mesh: grp: 2 (over x), pq: 16 (over z, y, core).
Axes of the slice: x: 2, y: 2, z: 4, core: 2. Of those that a mesh axis runs over, the one named last changes fastest.
Arguments:
- pair_blocks: bfloat16 [4, 288, 128, 128], P('grp', 'pq'), may hold values from -6 to 6
- block_list: int32 [4, 288], P('grp', 'pq'), may hold values from 0 to 2047, as said below
- block_count: int32 [4, 16], P('grp', 'pq'), may hold values from 1 to 18, as said below
- coef: bfloat16 [4096, 512], P('pq', 'grp'), may hold values from -0.09375 to 0.09375
Outputs:
- transformed: float32 [8, 512, 512], P('grp', 'pq')
The draws below stay inside these ranges and needn't reach their ends.
Inputs may be any that keep to these rules, and one draw needn't show every extreme that they name: `block_list`: within one row the ids are distinct, each in 0 to 2 * 32^2 - 1. `block_count`: in every row some device has exactly 18 live slots.
All inputs are finite; a program needn't handle non-finite values.
Results may differ from the reference program's by a relative error of at most 0.0042.
Values may be sent and summed in bfloat16 or wider, within the bound.
No kernel may reach another device: no remote copies, remote signals or barrier semaphores. Data moves between devices by JAX's collectives and lax.ppermute only.
A program may use at most 64 MiB of HBM per device.

```python
import jax
import jax.numpy as jnp
from jax import lax

NAO = 4096
NMO = 512
TILE = 128
KL_PANEL = 2
PANELS = 2
SLOTS = 18
NKL = 8
N_GRP = 2
N_PQ = 16


def draw_block_list(key, part):
    total_rows = PANELS * N_GRP
    keys = jax.random.split(jax.random.fold_in(key, 11), total_rows)
    idents = KL_PANEL * (NAO // TILE) * (NAO // TILE)

    def one_row(row_key):
        return jax.random.permutation(row_key, idents)[:N_PQ * SLOTS]
    return jax.vmap(one_row)(keys).astype(jnp.int32)


def draw_block_count(key, part):
    total_rows = PANELS * N_GRP
    first_key, second_key, third_key = jax.random.split(jax.random.fold_in(key, 23), 3)
    low = max(SLOTS // 2, 1)
    high = max(SLOTS, low + 1)
    first = jax.random.randint(first_key, (total_rows, N_PQ), low, high)
    second = jax.random.randint(second_key, (total_rows, N_PQ), low, high)
    counts = 1 + first * second // SLOTS
    counts = jnp.minimum(counts, SLOTS)
    busiest = jax.random.randint(third_key, (total_rows, 1), 0, N_PQ)
    places = jnp.arange(N_PQ, dtype=jnp.int32)[None, :]
    counts = jnp.where(places == busiest, SLOTS, counts)
    return counts.astype(jnp.int32)


def shard_levels(stream_key, shape, cuts, smallest, high):
    loudness, own = 1.0, jax.random.fold_in(stream_key, 6)
    for position, shards_of in cuts:
        steps = jnp.exp(jax.random.uniform(jax.random.fold_in(own, position), (shards_of,), jnp.float32, smallest / len(cuts), high / len(cuts)))
        loudness = loudness * jnp.repeat(steps, shape[position] // shards_of).reshape([-1 if axis == position else 1 for axis in range(len(shape))])
    return loudness


def scatter_about(stream_key, shape, width, most, cuts=(), kind=jnp.bfloat16):
    factor_of = shard_levels(stream_key, shape, cuts, -0.22, 0.18) if cuts else 1.0
    entries = jax.random.normal(stream_key, shape, jnp.float32) * width * factor_of
    return jnp.minimum(jnp.maximum(entries, -most), most).astype(kind)


def setup_inputs(seed: int = 0) -> dict:
    key_list = jax.random.split(jax.random.key(seed), 5)
    return {
        "pair_blocks": scatter_about(key_list[0], (PANELS * N_GRP, N_PQ * SLOTS, TILE, TILE), 1.0, 6.0, ((0, 2), (1, 16))),
        "block_list": draw_block_list(jax.random.fold_in(key_list[4], 71), 0),
        "block_count": draw_block_count(jax.random.fold_in(key_list[4], 71), 0),
        "coef": scatter_about(key_list[3], (NAO, NMO), NAO ** -0.5, 0.09375, ((0, 16), (1, 2))),
    }


def reference(pair_blocks, block_list, block_count, coef):
    nblk = NAO // TILE
    per_kl = nblk * nblk

    def one_row(inputs):
        blocks, idents, counts = inputs

        def step(acc, slot):
            live = (slot % SLOTS) < counts[slot // SLOTS]

            def add(total):
                ident = idents[slot]
                which = (ident // per_kl).astype(jnp.int32)
                row_blk = ((ident // nblk) % nblk).astype(jnp.int32)
                col_blk = (ident % nblk).astype(jnp.int32)
                col_coef = lax.dynamic_slice_in_dim(coef, col_blk * TILE, TILE, 0)
                row_coef = lax.dynamic_slice_in_dim(coef, row_blk * TILE, TILE, 0)
                block = lax.dynamic_index_in_dim(blocks, slot, 0, keepdims=False)
                half = jnp.dot(block, col_coef, preferred_element_type=jnp.float32).astype(jnp.bfloat16)
                term = jnp.dot(row_coef.T, half, preferred_element_type=jnp.float32)
                current = lax.dynamic_index_in_dim(total, which, 0, keepdims=False)
                return lax.dynamic_update_index_in_dim(total, current + term, which, 0)

            return lax.cond(live, add, lambda total: total, acc), None

        start = jnp.zeros((KL_PANEL, NMO, NMO), jnp.float32)
        result, _ = lax.scan(step, start, jnp.arange(N_PQ * SLOTS, dtype=jnp.int32))
        return result

    rows = lax.map(one_row, (pair_blocks, block_list, block_count))
    return rows.reshape(NKL, NMO, NMO)
```

```python
import functools

import jax
import jax.numpy as jnp
from jax import lax
from jax.experimental import pallas as pl
from jax.experimental.pallas import tpu as pltpu
from jax.sharding import PartitionSpec as P

KL_PANEL = 2
UNROLL = 2
CHUNK = 4


def block_term(block, ident, coef_full, tile, nblk):
    per_kl = nblk * nblk
    which = ident // per_kl
    row_blk = ident // nblk % nblk
    col_blk = ident % nblk
    col_coef = lax.dynamic_slice_in_dim(coef_full, col_blk * tile, tile, 0)
    row_coef = lax.dynamic_slice_in_dim(coef_full, row_blk * tile, tile, 0)
    half = jnp.dot(block, col_coef, preferred_element_type=jnp.float32).astype(jnp.bfloat16)
    term = lax.dot_general(
        row_coef, half, (((0,), (0,)), ((), ())), preferred_element_type=jnp.float32
    )
    return which, term


def general_body(pair_blocks, block_list, block_count, coef):
    coef_rows = lax.all_gather(coef, "pq", axis=0, tiled=True)
    coef_full = lax.all_gather(coef_rows, "grp", axis=1, tiled=True)
    tile = pair_blocks.shape[2]
    nblk = coef_full.shape[0] // tile
    width = coef_full.shape[1]
    pieces = []
    for panel in range(pair_blocks.shape[0]):

        def step(slot, total):
            which, term = block_term(
                pair_blocks[panel, slot], block_list[panel, slot], coef_full, tile, nblk
            )
            current = lax.dynamic_index_in_dim(total, which, 0, keepdims=False)
            return lax.dynamic_update_index_in_dim(total, current + term, which, 0)

        empty = jnp.zeros((KL_PANEL, width, width), jnp.float32)
        pieces.append(lax.fori_loop(0, block_count[panel, 0], step, empty))
    return lax.psum_scatter(jnp.concatenate(pieces, 0), "pq", scatter_dimension=1, tiled=True)


def permute(value, masks, places):
    pairs = [(place, place ^ masks[place & 1]) for place in range(places)]
    return lax.ppermute(value, ("grp", "pq"), pairs)


def mask_of(index, dims, side):
    mask = 0
    for bit, masks in enumerate(dims):
        if index >> bit & 1:
            mask ^= masks[side]
    return mask


def kernel(sizes, gather_dims, scatter_dims, *refs):
    own_meta, far_meta, own_blocks, far_blocks, own_coef, far_coef = refs[:6]
    outs = refs[6:-5]
    coef_t, coef_i, halves, lefts, total = refs[-5:]
    n_pq, tile, nblk, slots, rows, cols, out_rows = sizes
    panels = own_blocks.shape[0]
    width = coef_t.shape[0]
    per_kl = nblk * nblk
    pq = lax.axis_index("pq")
    me = lax.axis_index("grp") * n_pq + pq
    side = lax.rem(pq, 2)
    dump = halves.shape[1] - 1

    for source, base, is_far in ((own_coef, me, 0), (far_coef, me ^ 1, 1)):
        for piece in range(source.shape[0]):
            even = mask_of(piece, gather_dims, is_far)
            odd = mask_of(piece, gather_dims, 1 - is_far)
            place = base ^ jnp.where(side == 1, odd, even)
            top = pl.multiple_of(lax.div(place, n_pq) * cols, cols)
            start = pl.multiple_of(lax.rem(place, n_pq) * rows, rows)
            coef_t[pl.ds(top, cols), pl.ds(start, rows)] = source[piece]
    for chunk in range(coef_i.shape[0] // out_rows):
        owner = pq ^ jnp.where(side == 1, mask_of(chunk, scatter_dims, 1), mask_of(chunk, scatter_dims, 0))
        start = pl.multiple_of(owner * out_rows, out_rows)
        coef_i[chunk * out_rows:(chunk + 1) * out_rows, :] = coef_t[pl.ds(start, out_rows), :]

    for panel in range(panels):
        filled = (jnp.int32(0),) * KL_PANEL
        for meta, blocks in ((own_meta, own_blocks), (far_meta, far_blocks)):
            count = meta[panel, slots]

            def step(group, filled):
                for lane in range(UNROLL):
                    slot = group * UNROLL + lane
                    live = slot < count
                    slot = jnp.minimum(slot, slots - 1)
                    ident = meta[panel, slot]
                    which = lax.div(ident, per_kl)
                    row_blk = lax.rem(lax.div(ident, nblk), nblk)
                    col_blk = lax.rem(ident, nblk)
                    where = filled[0]
                    for kl in range(1, KL_PANEL):
                        where = jnp.where(which == kl, filled[kl], where)
                    where = jnp.where(live, where, dump)
                    filled = tuple(
                        n + jnp.where(live & (which == kl), 1, 0) for kl, n in enumerate(filled)
                    )
                    right = coef_t[:, pl.ds(pl.multiple_of(col_blk * tile, tile), tile)]
                    half = lax.dot_general(
                        blocks[panel, slot], right, (((1,), (1,)), ((), ())),
                        preferred_element_type=jnp.float32,
                    )
                    halves[which, where] = half.astype(jnp.bfloat16)
                    lefts[which, where] = coef_i[:, pl.ds(pl.multiple_of(row_blk * tile, tile), tile)]
                return filled

            filled = lax.fori_loop(0, lax.div(count + UNROLL - 1, UNROLL), step, filled)
        for kl in range(KL_PANEL):
            for extra in range(CHUNK - 1):
                halves[kl, filled[kl] + extra] = jnp.zeros(halves.shape[2:], halves.dtype)
                lefts[kl, filled[kl] + extra] = jnp.zeros(lefts.shape[2:], lefts.dtype)
            total[...] = jnp.zeros_like(total)

            def add(chunk, carry):
                base = chunk * CHUNK
                left = jnp.concatenate([lefts[kl, base + c] for c in range(CHUNK)], 1)
                right = jnp.concatenate([halves[kl, base + c] for c in range(CHUNK)], 0)
                total[...] += jnp.dot(left, right, preferred_element_type=jnp.float32)
                return carry

            lax.fori_loop(0, lax.div(filled[kl] + CHUNK - 1, CHUNK), add, 0)
            at = panel * KL_PANEL + kl
            begin = 0
            for out in outs:
                end = begin + out.shape[1]
                out[at] = total[begin:end].astype(out.dtype)
                begin = end


def fast_body(pair_blocks, block_list, block_count, coef):
    n_grp, n_pq = lax.axis_size("grp"), lax.axis_size("pq")
    places = n_grp * n_pq
    panels, slots, tile = pair_blocks.shape[:3]
    rows, cols = coef.shape
    nao, nmo = rows * n_pq, cols * n_grp
    out_rows = nmo // n_pq
    pq_masks = [2] + [(1 << b) | (1 << (b - 1) if b > 2 else 0) for b in range(2, n_pq.bit_length() - 1)]
    grp_masks = [n_pq << b for b in range(n_grp.bit_length() - 1)]
    y, x = pq_masks[0], grp_masks[0]
    gather_dims = [(m, m) for m in pq_masks[1:] + grp_masks[1:]] + [(x, y), (y, x)]
    order = [(m, m) for m in pq_masks]
    order[0], order[1] = (pq_masks[0], pq_masks[1]), (pq_masks[1], pq_masks[0])
    scatter_dims = order[::-1]

    meta = jnp.concatenate([block_list, block_count], 1)
    swap = (1, 1)
    far_blocks, far_meta = permute(pair_blocks, swap, places), permute(meta, swap, places)
    mine = coef.T[None]
    for masks in gather_dims:
        mine = jnp.concatenate([mine, permute(mine, masks, places)], 0)
    far = permute(mine, swap, places)

    total_rows = nmo // 2
    n_kl = panels * KL_PANEL
    sizes = (n_pq, tile, nao // tile, slots, rows, cols, out_rows)
    splits = [(out_rows, jnp.float32)]
    size = out_rows
    for level in range(len(order)):
        splits.append((size, jnp.bfloat16 if level == len(order) - 1 else jnp.float32))
        size *= 2
    cap = 2 * slots + CHUNK
    vmem, smem = pl.BlockSpec(memory_space=pltpu.VMEM), pl.BlockSpec(memory_space=pltpu.SMEM)
    flops = 2 * panels * slots * tile * (tile + total_rows) * nmo * 2
    outs = pl.pallas_call(
        functools.partial(kernel, sizes, gather_dims, scatter_dims),
        out_shape=[jax.ShapeDtypeStruct((n_kl, r, nmo), t) for r, t in splits],
        in_specs=[smem, smem, vmem, vmem, vmem, vmem],
        out_specs=[vmem] * len(splits),
        scratch_shapes=[
            pltpu.VMEM((nmo, nao), jnp.bfloat16),
            pltpu.VMEM((total_rows, nao), jnp.bfloat16),
            pltpu.VMEM((KL_PANEL, cap, tile, nmo), jnp.bfloat16),
            pltpu.VMEM((KL_PANEL, cap, total_rows, tile), jnp.bfloat16),
            pltpu.VMEM((total_rows, nmo), jnp.float32),
        ],
        cost_estimate=pl.CostEstimate(flops=flops, bytes_accessed=2 * nao * nmo, transcendentals=0),
        compiler_params=pltpu.CompilerParams(vmem_limit_bytes=48 << 20),
    )(meta, far_meta, pair_blocks, far_blocks, mine, far)
    keep, waiting = outs[0], list(outs[1:])
    received = []
    for masks in order:
        send = waiting.pop()
        at = send.shape[1]
        for part in received:
            send = send + part[:, at:2 * at].astype(jnp.float32)
        received.append(permute(send.astype(jnp.bfloat16), masks, places))
    for part in received:
        keep = keep + part[:, :out_rows].astype(jnp.float32)
    return keep


def suits_fast_path(mesh, shapes):
    n_grp, n_pq = mesh.shape["grp"], mesh.shape["pq"]
    rows, cols = shapes[3][0] // n_pq, shapes[3][1] // n_grp
    out_rows = shapes[3][1] // n_pq
    powers = all(n & (n - 1) == 0 for n in (n_grp, n_pq))
    return powers and n_grp >= 2 and n_pq >= 8 and rows % 128 == 0 and cols % 128 == 0 and out_rows % 16 == 0


def solution(mesh):
    in_specs = (P("grp", "pq", None, None), P("grp", "pq"), P("grp", "pq"), P("pq", "grp"))
    out_specs = P("grp", "pq", None)

    def run(*args):
        body = fast_body if suits_fast_path(mesh, [a.shape for a in args]) else general_body
        return jax.shard_map(body, mesh=mesh, in_specs=in_specs, out_specs=out_specs, check_vma=False)(*args)

    return run
```
